32 devices in a mesh: dp: 16 (over z, y, x), mp: 2 (over core).
Axes of the slice: x: 2, y: 2, z: 4, core: 2. Of those that a mesh axis runs over, the one named last changes fastest.
Arguments:
- features: bfloat16 [8192, 2048], P('dp', 'mp'), may hold values from -6 to 6
- gains: float32 [2, 2048], replicated, may hold values from 0.25 to 1.75
- weights: bfloat16 [2, 2048, 2048], P(None, None, 'mp'), may hold values from -0.125 to 0.125
- heads: bfloat16 [256, 32, 2048], P('dp', None, 'mp'), may hold values from -0.125 to 0.125
- lengths: int32 [16, 16], P('dp'), may hold values from 1 to 32, 256 in all within a row
- owners: int32 [16, 16], P('dp'), may hold values from 0 to 15, each once within a row
- labels: int32 [8192], P('dp'), may hold values from 0 to 31
Outputs:
- body_grads: float32 [2, 2048, 2048], P(None, 'dp', 'mp')
- token_loss: bfloat16 [8192], P('dp')
The draws below stay inside these ranges and needn't reach their ends.
Inputs may be any that keep to these rules, and one draw needn't show every extreme that they name: `lengths`: each row (one block's 16 clients) holds token counts of 1 to 32 that sum to 256; some client of each block holds exactly 32. `owners`: each row names every head owner 0 to 15 exactly once.
All inputs are finite; a program needn't handle non-finite values.
Results may differ from the reference program's by a relative error of at most 0.0073.
Values may be sent and summed in bfloat16 or wider, within the bound.
No kernel may reach another device: no remote copies, remote signals or barrier semaphores. Data moves between devices by JAX's collectives and lax.ppermute only.
A program may use at most 128 MiB of HBM per device.

```python
import math
import jax
import jax.numpy as jnp
import numpy as np
from jax import lax

D = 2048
CLASSES = 32
TOK_DEV = 512
MOST = 32
CLIENTS = 256
TOKENS = 8192
N_DP = 16


def place_ends(array, key, least, top_value):
    longest = array.shape.index(max(array.shape))
    spots = []
    for shift in (0, 1):
        where = [jax.random.randint(jax.random.fold_in(key, axis), (), 0, length) for axis, length in enumerate(array.shape)]
        where[longest] = (where[longest] + shift) % array.shape[longest]
        spots.append(tuple(where))
    return array.at[spots[0]].set(least).at[spots[1]].set(top_value)


def steps_of(stream_key, dims, pieces, least, largest):
    gain = 1.0
    for position, shards_of in pieces:
        heights = jax.random.uniform(jax.random.fold_in(jax.random.fold_in(stream_key, 6), position), (shards_of,), jnp.float32, least / len(pieces), largest / len(pieces))
        gain = gain * jnp.repeat(jnp.exp(heights), dims[position] // shards_of).reshape((-1,) + (1,) * (len(dims) - 1 - position))
    return gain


def length_profile(number_of, total, limit, skew):
    loads = [(1 << 20) // math.isqrt(rank ** skew) + 1 for rank in range(2, number_of + 1)]
    rest, given = total - limit - (number_of - 1), [1] * (number_of - 1)
    while rest > 0:
        free = [i for i in range(number_of - 1) if given[i] < limit]
        whole, remaining = sum([loads[i] for i in free]), rest
        for i in free:
            more = min(limit - given[i], max(1, remaining * loads[i] // whole), rest)
            given[i] = given[i] + more
            rest = rest - more
    return np.array([limit] + given)


def uneven_parts(key, count, total, reach, lean):
    if count == 2:
        one = jax.random.randint(key, (), max(1, total - reach), min(reach, total - 1) + 1)
        return jnp.stack([one, total - one])
    sizes = jnp.asarray(length_profile(count, total, reach, lean), jnp.int32)
    twos = (count - 1) // 2
    donor, receiver = sizes[1:1 + 2 * twos:2], sizes[2:2 + 2 * twos:2]
    slack = jnp.minimum(donor - 1, reach - receiver)
    passed = jax.random.randint(jax.random.fold_in(key, 1), (twos,), 0, 1 << 20) % (slack + 1)
    sizes = sizes.at[1:1 + 2 * twos:2].set(donor - passed).at[2:2 + 2 * twos:2].set(receiver + passed)
    return sizes[jax.random.permutation(jax.random.fold_in(key, 2), count)]


def centred(key, extent, width, bound, shards=(), kind=jnp.bfloat16):
    factor_of = steps_of(key, extent, shards, -0.22, 0.18) if shards else 1.0
    values = jax.random.normal(key, extent, jnp.float32) * width * factor_of
    return jnp.minimum(jnp.maximum(values, -bound), bound).astype(kind)


def setup_inputs(seed: int = 0) -> dict:
    arg_keys = jax.random.split(jax.random.key(seed), 8)
    return {
        "features": centred(arg_keys[0], (TOKENS, D), 1.0, 6.0, ((0, 16), (1, 2))),
        "gains": jnp.clip(1.0 + 0.15 * jax.random.normal(arg_keys[1], (2, D), jnp.float32), 0.25, 1.75),
        "weights": centred(arg_keys[2], (2, D, D), D ** -0.5, 0.125, ((2, 2),)),
        "heads": centred(arg_keys[3], (CLIENTS, CLASSES, D), D ** -0.5, 0.125, ((0, 16), (2, 2))),
        "lengths": jax.vmap(lambda own: uneven_parts(own, N_DP, TOK_DEV // 2, MOST, 2))(jax.random.split(arg_keys[4], N_DP)).reshape((N_DP, N_DP)).astype(jnp.int32),
        "owners": jax.vmap(lambda own: jax.random.permutation(own, N_DP))(jax.random.split(arg_keys[5], N_DP)).reshape((N_DP, N_DP)).astype(jnp.int32),
        "labels": place_ends(jax.random.randint(arg_keys[6], (TOKENS,), 0, CLASSES), jax.random.fold_in(arg_keys[6], 1), 0, CLASSES - 1).astype(jnp.int32),
    }


EPSILON = 1e-06

def norm_layer(inputs, norm_gain, weight):
    widened = inputs.astype(jnp.float32)
    rms_scale = lax.rsqrt(lax.optimization_barrier(jnp.mean(widened * widened, -1, keepdims=True)) + EPSILON)
    normed = (widened * rms_scale * norm_gain).astype(jnp.bfloat16)
    pre_act = jnp.dot(normed, weight, preferred_element_type=jnp.float32)
    outputs = (widened + jax.nn.gelu(pre_act)).astype(jnp.bfloat16)
    return (normed, rms_scale, pre_act, outputs)

def gelu_back(pre_act, upstream):
    return jax.vjp(jax.nn.gelu, pre_act)[1](upstream)[0]

def loss_terms(logits, slot_labels, slot_lens):
    class_ids = lax.broadcasted_iota(jnp.int32, logits.shape, 2)
    class_hit = class_ids == slot_labels[..., None]
    log_total = jnp.log(lax.optimization_barrier(jnp.sum(jnp.exp(logits), -1)))
    picked = lax.optimization_barrier(jnp.sum(jnp.where(class_hit, logits, 0.0), -1))
    slot_live = slot_lens > 0
    losses = jnp.where(slot_live, log_total - picked, 0.0)
    weight_tok = jnp.where(slot_live, 1.0 / jnp.maximum(slot_lens, 1).astype(logits.dtype), 0.0)
    softmax_probs = jnp.exp(logits - log_total[..., None])
    dlogits = ((softmax_probs - class_hit.astype(logits.dtype)) * weight_tok[..., None]).astype(jnp.bfloat16)
    return (losses.astype(jnp.bfloat16), dlogits)

def reference(features, gains, weights, heads, lengths, owners, labels):
    normed_first, scale_first, pre_first, hidden_mid = norm_layer(features, gains[0], weights[0])
    normed_second, scale_second, pre_second, hidden_top = norm_layer(hidden_mid, gains[1], weights[1])
    heads_grid = heads.reshape(N_DP, N_DP, CLASSES, D)

    def device_heads(device_item):
        slot_source, dev_labels, dev_lengths, dev_owners, source = device_item
        client_ends = jnp.cumsum(dev_lengths).astype(jnp.int32)
        starts = (client_ends - dev_lengths).astype(jnp.int32)
        offsets = jnp.arange(MOST, dtype=jnp.int32)
        slot_live = offsets[None, :] < dev_lengths[:, None]
        slot_index = jnp.where(slot_live, starts[:, None] + offsets[None, :], TOK_DEV).reshape(-1).astype(jnp.int32)
        safe_index = jnp.minimum(slot_index, TOK_DEV - 1).astype(jnp.int32)
        slot_feats = slot_source[safe_index].reshape(N_DP, MOST, D).astype(jnp.float32)
        slot_heads = heads_grid[dev_owners, source].astype(jnp.float32)
        logits = jnp.einsum('jmd,jcd->jmc', slot_feats, slot_heads)
        slot_labels = dev_labels[safe_index].reshape(N_DP, MOST)
        slot_lens = jnp.where(slot_live, dev_lengths[:, None], 0)
        losses, dlogits = loss_terms(logits, slot_labels, slot_lens)
        slot_grads = jnp.einsum('jmc,jcd->jmd', dlogits.astype(jnp.float32), slot_heads).astype(jnp.bfloat16)
        tok_grads = jnp.zeros((TOK_DEV, D), jnp.bfloat16).at[slot_index].add(slot_grads.reshape(-1, D), mode='drop')
        tok_loss = jnp.zeros((TOK_DEV,), jnp.bfloat16).at[slot_index].add(losses.reshape(-1), mode='drop')
        return (tok_grads, tok_loss)
    tok_grads, tok_loss = lax.map(device_heads, (hidden_top.reshape(N_DP, TOK_DEV, D), labels.reshape(N_DP, TOK_DEV), lengths, owners, jnp.arange(N_DP, dtype=jnp.int32)))
    upstream = tok_grads.reshape(TOKENS, D).astype(jnp.float32)
    delta_second = gelu_back(pre_second, upstream).astype(jnp.bfloat16)
    grad_second = lax.dot_general(normed_second, delta_second, (((0,), (0,)), ((), ())), preferred_element_type=jnp.float32)
    dnormed = jnp.dot(delta_second, weights[1].T, preferred_element_type=jnp.float32)
    widened = hidden_mid.astype(jnp.float32)
    cross_term = lax.optimization_barrier(jnp.mean(widened * gains[1] * dnormed, -1, keepdims=True))
    dhidden = upstream + gains[1] * scale_second * dnormed - widened * scale_second ** 3 * cross_term
    delta_first = gelu_back(pre_first, dhidden).astype(jnp.bfloat16)
    grad_first = lax.dot_general(normed_first, delta_first, (((0,), (0,)), ((), ())), preferred_element_type=jnp.float32)
    return (jnp.stack([grad_first, grad_second]), tok_loss.reshape(TOKENS))
```

```python
import jax
import jax.numpy as jnp
from jax import lax
from jax.sharding import PartitionSpec as P

EPSILON = 1e-06
PLANE = 4


def gelu_slope(pre):
    return jax.vjp(jax.nn.gelu, pre)[1](jnp.ones_like(pre))[0]


def swap_cores(value):
    return lax.ppermute(value, "mp", [(0, 1), (1, 0)])


def xor_send(value, mask, count):
    return lax.ppermute(value, "dp", [(i, i ^ mask) for i in range(count)])


def strip_order(count):
    if count == 1:
        return [0]
    kept = [2 * item for item in strip_order(count // 2)]
    return [item + 1 for item in kept] + kept


def join_cores(own, other, core):
    return jnp.where(
        core == 0,
        jnp.concatenate([own, other], 1),
        jnp.concatenate([other, own], 1),
    )


def norm_layer(full_rows, own_cols, norm_gain, weight):
    widened = full_rows.astype(jnp.float32)
    scale = lax.rsqrt(jnp.mean(widened * widened, -1, keepdims=True) + EPSILON)
    normed = (widened * scale * norm_gain).astype(jnp.bfloat16)
    pre = jnp.dot(normed, weight, preferred_element_type=jnp.float32)
    out = (own_cols.astype(jnp.float32) + jax.nn.gelu(pre)).astype(jnp.bfloat16)
    return normed, scale, pre, out


def strips_for(normed, plane_to, outer, count):
    rows = normed.shape[1] // count
    parts = [
        lax.dynamic_slice_in_dim(normed, ((outer ^ j) * PLANE + plane_to) * rows, rows, 1)
        for j in strip_order(count // PLANE)
    ]
    return jnp.concatenate(parts, 1)


def contract_rows(left, right):
    return lax.dot_general(
        left, right, (((0,), (0,)), ((), ())), preferred_element_type=jnp.float32
    )


def weight_grad(strips, delta, count):
    half = delta.shape[0] // 2
    from_x = xor_send(delta, 1, count)
    from_y = xor_send(delta, 2, count)
    corner_head = xor_send(from_x[:half], 2, count)
    corner_tail = xor_send(from_y[half:], 1, count)
    partial = contract_rows(
        jnp.concatenate([strips[0], strips[1], strips[2], strips[3]], 0),
        jnp.concatenate([delta, from_x, from_y, corner_head, corner_tail], 0),
    )
    step = PLANE
    while step < count:
        half_rows = partial.shape[0] // 2
        arrived = xor_send(partial[:half_rows].astype(jnp.bfloat16), step, count)
        partial = partial[half_rows:] + arrived.astype(jnp.float32)
        step *= 2
    return partial


def body(features, gains, weights, heads, lengths, owners, labels):
    count = lax.axis_size("dp")
    core = lax.axis_index("mp")
    device = lax.axis_index("dp")
    plane, outer = device % PLANE, device // PLANE
    slots, width = features.shape
    tok = slots // 2
    classes = heads.shape[1]
    moved = lax.all_to_all(heads, "dp", split_axis=0, concat_axis=0, tiled=True)
    own = features[:tok]
    rows_first = join_cores(own, swap_cores(own), core)
    full_width = rows_first.shape[1]
    normed_first, _, pre_first, mid = norm_layer(rows_first, own, gains[0], weights[0])
    rows_second = join_cores(mid, swap_cores(mid), core)
    normed_second, scale, pre_second, top = norm_layer(rows_second, mid, gains[1], weights[1])
    strips_first, strips_second = (
        [
            strips_for(normed, plane, outer, count),
            *(xor_send(strips_for(normed, plane ^ k, outer, count), k, count) for k in (1, 2, 3)),
        ]
        for normed in (normed_first, normed_second)
    )
    client_lens, client_owners = lengths[0], owners[0]
    ends = jnp.cumsum(client_lens)
    starts = ends - client_lens
    matches = client_owners[None, :] == lax.broadcasted_iota(jnp.int32, (count, count), 0)
    first = jnp.sum(jnp.where(matches, starts[None, :], 0), 1)
    lens = jnp.sum(jnp.where(matches, client_lens[None, :], 0), 1)
    position = lax.broadcasted_iota(jnp.int32, (count, tok), 1)
    mine = (position >= first[:, None]) & (position < (first + lens)[:, None])
    tok_len = jnp.sum(jnp.where(mine, lens[:, None], 0), 0)
    live = tok_len > 0
    all_heads = moved.reshape(count * classes, width)
    shares = lax.dot_general(
        all_heads, top, (((1,), (1,)), ((), ())), preferred_element_type=jnp.float32
    ).reshape(count, classes, tok)
    share = jnp.sum(jnp.where(mine[:, None, :], shares, 0.0), 0)
    logits = share + swap_cores(share)
    hit = lax.broadcasted_iota(jnp.int32, (classes, tok), 0) == labels[None, :tok]
    log_total = jnp.log(jnp.sum(jnp.exp(logits), 0))
    picked = jnp.sum(jnp.where(hit, logits, 0.0), 0)
    losses = jnp.where(live, log_total - picked, 0.0).astype(jnp.bfloat16)
    per_tok = jnp.where(live, 1.0 / jnp.maximum(tok_len, 1).astype(jnp.float32), 0.0)
    dlogits = ((jnp.exp(logits - log_total) - hit.astype(jnp.float32)) * per_tok).astype(
        jnp.bfloat16
    )
    spread = jnp.where(mine[:, None, :], dlogits[None], jnp.bfloat16(0)).reshape(-1, tok)
    upstream = contract_rows(spread, all_heads).astype(jnp.bfloat16).astype(jnp.float32)
    delta_second = (upstream * gelu_slope(pre_second)).astype(jnp.bfloat16)
    grad_second = weight_grad(strips_second, delta_second, count)
    cross = jnp.sum(delta_second.astype(jnp.float32) * pre_second, -1)
    cross = (cross + swap_cores(cross)) / full_width
    start = core * width
    other_start = (1 - core) * width
    own_rows = lax.dynamic_slice_in_dim(weights[1], start, width, 0)
    other_rows = lax.dynamic_slice_in_dim(weights[1], other_start, width, 0)
    turned = (((1,), (1,)), ((), ()))
    sent = lax.dot_general(
        delta_second, other_rows, turned, preferred_element_type=jnp.float32
    ).astype(jnp.bfloat16)
    kept = lax.dot_general(delta_second, own_rows, turned, preferred_element_type=jnp.float32)
    dnormed = kept + swap_cores(sent).astype(jnp.float32)
    gain_cols = lax.dynamic_slice_in_dim(gains[1], start, width, 0)
    dhidden = (
        upstream
        + gain_cols * scale * dnormed
        - mid.astype(jnp.float32) * scale**2 * cross[:, None]
    )
    delta_first = (dhidden * gelu_slope(pre_first)).astype(jnp.bfloat16)
    grad_first = weight_grad(strips_first, delta_first, count)
    tok_loss = jnp.concatenate([losses, jnp.zeros((slots - tok,), jnp.bfloat16)])
    return (jnp.stack([grad_first, grad_second]), tok_loss)


def solution(mesh):
    return jax.shard_map(
        body,
        mesh=mesh,
        in_specs=(
            P("dp", "mp"),
            P(),
            P(None, None, "mp"),
            P("dp", None, "mp"),
            P("dp", None),
            P("dp", None),
            P("dp"),
        ),
        out_specs=(P(None, "dp", "mp"), P("dp")),
        check_vma=False,
    )
```
